32 devices in a mesh: inner: 4 (over z), outer: 8 (over y, x, core).
Axes of the slice: x: 2, y: 2, z: 4, core: 2. Of those that a mesh axis runs over, the one named last changes fastest.
Arguments:
- inner_state: float32 [2, 16, 2048], P(None, 'inner', 'outer'), may hold values from -6 to 6
- outer_state: float32 [2, 640, 4096], P(None, 'inner', 'outer'), may hold values from -6 to 6
- energies: float32 [16, 2048], P('inner', 'outer'), may hold values from -2 to 2
- dipole: float32 [16, 2048, 2048], P('inner', 'outer'), may hold values from -0.125 to 0.125
- surface: float32 [16, 40, 2048], P('inner', None, 'outer'), may hold values from -0.125 to 0.125
- thresholds: float32 [640], P('inner'), may hold values from 0 to 2
- coupling_coef: float32 [16, 40, 40], P('inner'), may hold values from -1 to 1
- coupling_pattern: int32 [16, 40, 40], P('inner'), may hold values 0 or 1
- block_sizes: int32 [16], P('inner'), may hold values from 1 to 2048, 30720 in all
- field_strength: float32 [2], replicated, may hold values from 0.5 to 2
Outputs:
- inner_final: float32 [2, 16, 2048], P(None, 'inner', 'outer')
- outer_final: float32 [2, 640, 4096], P(None, 'inner', 'outer')
The draws below stay inside these ranges and needn't reach their ends.
All inputs are finite; a program needn't handle non-finite values. No bound on the sum of `coupling_pattern` or of `block_sizes` on one device may be relied on, other than what follows from the above.
Results may differ from the reference program's by a relative error of at most 0.0001.
Values sent between devices are 32-bit elements; how exact they have to be, the bound alone decides.
A program may use at most 128 MiB of HBM per device.

```python
import math
import jax
import jax.numpy as jnp
import numpy as np
from jax import lax

BMAX = 2048
CHL = 40
STEPS = 2
ORDER = 4
NL = 16
NC = 640
NR = 4096


def touch_ends(entries, key, low, high):
    longest = entries.shape.index(max(entries.shape))
    spots = []
    for shift in (0, 1):
        where = [jax.random.randint(jax.random.fold_in(key, axis), (), 0, length) for axis, length in enumerate(entries.shape)]
        where[longest] = (where[longest] + shift) % entries.shape[longest]
        spots.append(tuple(where))
    return entries.at[spots[0]].set(low).at[spots[1]].set(high)


def shard_levels(rng, extent, split, least, largest):
    factor_of, own = 1.0, jax.random.fold_in(rng, 6)
    for position, parts in split:
        draws = jnp.exp(jax.random.uniform(jax.random.fold_in(own, position), (parts,), jnp.float32, least / len(split), largest / len(split)))
        factor_of = factor_of * jnp.repeat(draws, extent[position] // parts).reshape([-1 if axis == position else 1 for axis in range(len(extent))])
    return factor_of


def length_profile(amount, total, reach, lean):
    loads = [(1 << 20) // math.isqrt(rank ** lean) + 1 for rank in range(2, amount + 1)]
    surplus, given = total - reach - (amount - 1), [1] * (amount - 1)
    while surplus > 0:
        free = [i for i in range(amount - 1) if given[i] < reach]
        whole, left = sum([loads[i] for i in free]), surplus
        for i in free:
            addition = min(reach - given[i], max(1, left * loads[i] // whole), surplus)
            given[i] = given[i] + addition
            surplus = surplus - addition
    return np.array([reach] + given)


def ragged(stream_key, amount, total, reach, slope):
    if amount == 2:
        one = jax.random.randint(stream_key, (), max(1, total - reach), min(reach, total - 1) + 1)
        return jnp.stack([one, total - one])
    sizes = jnp.asarray(length_profile(amount, total, reach, slope), jnp.int32)
    pairs = (amount - 1) // 2
    giver, taker = sizes[1:1 + 2 * pairs:2], sizes[2:2 + 2 * pairs:2]
    room = jnp.minimum(giver - 1, reach - taker)
    shifted = jax.random.randint(jax.random.fold_in(stream_key, 1), (pairs,), 0, 1 << 20) % (room + 1)
    sizes = sizes.at[1:1 + 2 * pairs:2].set(giver - shifted).at[2:2 + 2 * pairs:2].set(taker + shifted)
    return sizes[jax.random.permutation(jax.random.fold_in(stream_key, 2), amount)]


def bell_draw(stream_key, shape, width, limit, split=(), held_as=jnp.bfloat16):
    result = width * jax.random.normal(stream_key, shape, jnp.float32)
    if split:
        result = result * shard_levels(stream_key, shape, split, -0.22, 0.18)
    return jnp.clip(result, -limit, limit).astype(held_as)


def setup_inputs(seed: int = 0) -> dict:
    streams_of = jax.random.split(jax.random.key(seed), 11)
    inner_state = bell_draw(streams_of[0], (2, NL, BMAX), 1.0, 6.0, ((1, 4), (2, 8)), jnp.float32)
    outer_state = bell_draw(streams_of[1], (2, NC, NR), 1.0, 6.0, ((1, 4), (2, 8)), jnp.float32)
    energies = jnp.clip(jax.random.uniform(streams_of[2], (NL, BMAX), jnp.float32, -2.0, 2.0) * shard_levels(streams_of[2], (NL, BMAX), ((0, 4), (1, 8)), -0.4, 0.0), -2.0, 2.0)
    dipole = bell_draw(streams_of[3], (NL, BMAX, BMAX), BMAX ** -0.5, 0.125, ((0, 4), (1, 8)), jnp.float32)
    surface = bell_draw(streams_of[4], (NL, CHL, BMAX), BMAX ** -0.5, 0.125, ((0, 4), (2, 8)), jnp.float32)
    thresholds = jnp.clip(2.0 * jax.random.uniform(streams_of[5], (NC,), jnp.float32) ** shard_levels(streams_of[5], (NC,), ((0, 4),), -0.2, 0.2), 0.0, 2.0)
    coupling_coef = bell_draw(streams_of[6], (NL, CHL, CHL), CHL ** -0.5, 1.0, ((0, 4),), jnp.float32)
    coupling_pattern = touch_ends((jax.random.randint(streams_of[7], (NL, CHL, CHL), 0, 2) < 1).astype(jnp.int32), jax.random.fold_in(streams_of[7], 1), 0, 1)
    block_sizes = ragged(streams_of[8], NL, NL * BMAX * 15 // 16, BMAX, 2).astype(jnp.int32)
    field_strength = jnp.clip(jax.random.uniform(streams_of[9], (STEPS,), jnp.float32, 0.5, 2.0), 0.5, 2.0)
    return dict(inner_state=inner_state, outer_state=outer_state, energies=energies, dipole=dipole, surface=surface, thresholds=thresholds, coupling_coef=coupling_coef, coupling_pattern=coupling_pattern, block_sizes=block_sizes, field_strength=field_strength)


kinetic_scale = 3.125
time_step = 0.1


def apply_operator(inner_part, outer_part, live_rows, energies, dipole, surface, thresholds, coupling, strength):
    highest = lax.Precision.HIGHEST
    forward = jnp.einsum('lij,plj->pli', dipole[:-1], inner_part[:, 1:], precision=highest)
    backward = jnp.einsum('lji,plj->pli', dipole[:-1], inner_part[:, :-1], precision=highest)
    zero_block = jnp.zeros((2, 1, BMAX), jnp.float32)
    forward = jnp.concatenate([forward, zero_block], axis=1)
    backward = jnp.concatenate([zero_block, backward], axis=1)
    first_point = outer_part[:, :, 0].reshape(2, NL, CHL)
    surf_term = jnp.einsum('lcs,plc->pls', surface, first_point, precision=highest)
    inner_image = live_rows * (energies * inner_part + strength * (forward + backward) - kinetic_scale * surf_term)
    boundary = jnp.einsum('lcs,pls->plc', surface, inner_part, precision=highest).reshape(2, NC)
    zero_col = jnp.zeros((2, NC, 1), jnp.float32)
    left_cells = jnp.concatenate([boundary[:, :, None], outer_part[:, :, :-1]], axis=2)
    right_cells = jnp.concatenate([outer_part[:, :, 1:], zero_col], axis=2)
    kinetic = kinetic_scale * (2.0 * outer_part - left_cells - right_cells)
    channel_grid = outer_part.reshape(2, NL, CHL, NR)
    upward = jnp.einsum('lab,plbr->plar', coupling[:-1], channel_grid[:, 1:], precision=highest)
    downward = jnp.einsum('lba,plbr->plar', coupling[:-1], channel_grid[:, :-1], precision=highest)
    zero_grid = jnp.zeros((2, 1, CHL, NR), jnp.float32)
    upward = jnp.concatenate([upward, zero_grid], axis=1)
    downward = jnp.concatenate([zero_grid, downward], axis=1)
    outer_image = kinetic + thresholds[None, :, None] * outer_part + strength * (upward + downward).reshape(2, NC, NR)
    return inner_image, outer_image


def reference(inner_state, outer_state, energies, dipole, surface, thresholds, coupling_coef, coupling_pattern, block_sizes, field_strength):
    positions = jnp.arange(BMAX, dtype=jnp.int32)
    live_rows = (positions[None, :] < block_sizes[:, None]).astype(jnp.float32)
    coupling = coupling_coef * coupling_pattern.astype(jnp.float32)
    current = (inner_state * live_rows, outer_state)
    for time_index in range(STEPS):
        strength = field_strength[time_index]
        taylor_term = current
        accumulated = current
        for power in range(1, ORDER + 1):
            inner_image, outer_image = apply_operator(taylor_term[0], taylor_term[1], live_rows, energies, dipole, surface, thresholds, coupling, strength)
            factor = time_step / power
            taylor_term = (factor * jnp.stack([inner_image[1], -inner_image[0]]), factor * jnp.stack([outer_image[1], -outer_image[0]]))
            accumulated = (accumulated[0] + taylor_term[0], accumulated[1] + taylor_term[1])
        current = accumulated
    return current[0], current[1]
```

```python
import functools

import jax
import jax.numpy as jnp
from jax import lax
from jax.experimental import pallas as pl
from jax.experimental.pallas import tpu as pltpu
from jax.sharding import PartitionSpec as P

STEPS = 2
ORDER = 4

kinetic_scale = 3.125
time_step = 0.1

MESH = pl.DeviceIdType.MESH
f32 = jnp.float32
bf16 = jnp.bfloat16
NT = (((1,), (1,)), ((), ()))
NN = (((1,), (0,)), ((), ()))


def split(x):
    high = x.astype(bf16)
    return high, (x - high.astype(f32)).astype(bf16)


def kernel(
    planes,
    sectors,
    ch,
    inner_ref,
    outer_ref,
    live_ref,
    energy_ref,
    dipole_ref,
    surface_ref,
    diag_ref,
    mix_ref,
    field_ref,
    inner_out,
    outer_out,
    dip_hi,
    dip_lo,
    mix_split,
    grid,
    term,
    peer_in,
    above_in,
    part_out,
    part_in,
    below_in,
    mixed,
    sem_a_send,
    sem_a_recv,
    sem_z_send,
    sem_z_recv,
    sem_b_send,
    sem_b_recv,
    sem_y_send,
    sem_y_recv,
    sem_up_send,
    sem_up_recv,
    sem_down_send,
    sem_down_recv,
):
    z = lax.axis_index("inner")
    me = lax.axis_index("outer")
    rows, rc = inner_ref.shape
    blocks = rows // 2
    nc, nr = outer_ref.shape[1:]
    total = rc * sectors
    width = peer_in.shape[3]
    has_below = z > 0
    has_above = z < planes - 1

    @pl.when(z == 0)
    def _():
        below_in[...] = jnp.zeros_like(below_in)
        grid[:, :, 0:ch, :] = jnp.zeros((2, 2, ch, nr), f32)

    @pl.when(z == planes - 1)
    def _():
        above_in[...] = jnp.zeros_like(above_in)
        grid[:, :, ch + nc : 2 * ch + nc, :] = jnp.zeros((2, 2, ch, nr), f32)

    term[...] = inner_ref[...] * live_ref[...]
    inner_out[...] = term[...]
    for p in range(2):
        x = outer_ref[p]
        grid[0, p, ch : ch + nc, :] = x
        outer_out[p] = x
    mh, ml = split(mix_ref[...])
    mix_split[0:nc, :] = mh
    mix_split[nc : 2 * nc, :] = ml

    def split_rows(i, carry):
        at = pl.ds(pl.multiple_of(i * 16, 16), 16)
        high, low = split(dipole_ref[at, :])
        dip_hi[at, :] = high
        dip_lo[at, :] = low
        return carry

    lax.fori_loop(0, blocks * rc // 16, split_rows, 0)

    eye = lax.broadcasted_iota(jnp.int32, (nc, width), 0) == lax.broadcasted_iota(
        jnp.int32, (nc, width), 1
    )

    def to_row(col):
        return jnp.sum(jnp.where(eye, col, 0.0), axis=0, keepdims=True)

    def to_col(row):
        return jnp.sum(jnp.where(eye, row, 0.0), axis=1, keepdims=True)

    def wait(ref, sem):
        pltpu.make_async_copy(ref, ref, sem).wait()

    def apply(t, carry):
        par = lax.rem(t, 2)
        nxt = 1 - par
        order = lax.rem(t, ORDER)
        strength = field_ref[lax.div(t, ORDER)]
        factor = time_step / (order + 1).astype(f32)
        last = order == ORDER - 1

        up = pltpu.make_async_remote_copy(
            src_ref=grid.at[par, :, pl.ds(nc, ch), :],
            dst_ref=grid.at[par, :, pl.ds(0, ch), :],
            send_sem=sem_up_send,
            recv_sem=sem_up_recv.at[par],
            device_id={"inner": z + 1, "outer": me},
            device_id_type=MESH,
        )
        down = pltpu.make_async_remote_copy(
            src_ref=grid.at[par, :, pl.ds(ch, ch), :],
            dst_ref=grid.at[par, :, pl.ds(ch + nc, ch), :],
            send_sem=sem_down_send,
            recv_sem=sem_down_recv.at[par],
            device_id={"inner": z - 1, "outer": me},
            device_id_type=MESH,
        )

        c = term[...]
        peer_in[par, me, 0:rows, 0:rc] = c
        edge_rows = []
        for p in range(2):
            edge_rows.append(to_row(grid[par, p, ch : ch + nc, 0:1]))
        for p in range(2):
            edge_rows.append(to_row(grid[par, p, ch : ch + nc, nr - 1 : nr]))
        for p in range(2):
            spread = jnp.concatenate(
                [
                    jnp.broadcast_to(c[2 * l + p : 2 * l + p + 1], (ch, rc))
                    for l in range(blocks)
                ],
                axis=0,
            )
            edge_rows.append(
                to_row(jnp.sum(surface_ref[...] * spread, axis=1, keepdims=True))
            )
        edge_rows.append(jnp.zeros((2, width), f32))
        peer_in[par, me, rows : rows + 8, :] = jnp.concatenate(edge_rows, axis=0)

        def send_a(s, k):
            to = lax.rem(me + s, sectors)
            pltpu.make_async_remote_copy(
                src_ref=peer_in.at[par, me],
                dst_ref=peer_in.at[par, me],
                send_sem=sem_a_send,
                recv_sem=sem_a_recv.at[par],
                device_id={"inner": z, "outer": to},
                device_id_type=MESH,
            ).start()
            return k

        lax.fori_loop(1, sectors, send_a, 0)

        @pl.when(has_below)
        def _():
            def send_z(s, k):
                to = lax.rem(me + s, sectors)
                pltpu.make_async_remote_copy(
                    src_ref=peer_in.at[par, me, pl.ds(0, rows), pl.ds(0, rc)],
                    dst_ref=above_in.at[par, me],
                    send_sem=sem_z_send,
                    recv_sem=sem_z_recv.at[par],
                    device_id={"inner": z - 1, "outer": to},
                    device_id_type=MESH,
                ).start()
                return k

            lax.fori_loop(0, sectors, send_z, 0)
            down.start()

        row_block = lax.broadcasted_iota(jnp.int32, (rows, 1), 0) // 2
        ch_, cl_ = split(c)
        both = jnp.concatenate([ch_, cl_], axis=0)
        back = jnp.zeros((rows, total), f32)
        for l in range(blocks):
            at = pl.ds(l * rc, rc)
            r = lax.dot_general(both, dip_hi[at, :], NN, preferred_element_type=f32)
            q = lax.dot_general(ch_, dip_lo[at, :], NN, preferred_element_type=f32)
            back = jnp.where(row_block == l, r[:rows] + r[rows:] + q, back)
        back = pltpu.roll(back, 2, 0)
        for k in range(sectors):
            part_out[k] = back[:, k * rc : (k + 1) * rc]
        part_in[par, me] = part_out[me]

        @pl.when(has_above)
        def _():
            def send_y(s, k):
                to = lax.rem(me + s, sectors)
                pltpu.make_async_remote_copy(
                    src_ref=part_out.at[to],
                    dst_ref=below_in.at[par, me],
                    send_sem=sem_y_send,
                    recv_sem=sem_y_recv.at[par],
                    device_id={"inner": z + 1, "outer": to},
                    device_id_type=MESH,
                ).start()
                return k

            lax.fori_loop(0, sectors, send_y, 0)
            up.start()

        def send_b(s, k):
            to = lax.rem(me + s, sectors)
            pltpu.make_async_remote_copy(
                src_ref=part_out.at[to],
                dst_ref=part_in.at[par, me],
                send_sem=sem_b_send,
                recv_sem=sem_b_recv.at[par],
                device_id={"inner": z, "outer": to},
                device_id_type=MESH,
            ).start()
            return k

        lax.fori_loop(1, sectors, send_b, 0)

        wait(peer_in.at[par, pl.ds(0, sectors - 1)], sem_a_recv.at[par])

        @pl.when(has_above)
        def _():
            wait(above_in.at[par], sem_z_recv.at[par])

        def forward_rows(values, l):
            vh, vl = values
            at = pl.ds(l * rc, rc)
            r = lax.dot_general(
                jnp.concatenate([vh, vl], axis=0), dip_hi[at, :], NT, preferred_element_type=f32
            )
            q = lax.dot_general(vh, dip_lo[at, :], NT, preferred_element_type=f32)
            return r[:rows] + r[rows:] + q

        own = split(
            jnp.concatenate([peer_in[par, k, 0:rows, 0:rc] for k in range(sectors)], axis=1)
        )
        other = split(jnp.concatenate([above_in[par, k] for k in range(sectors)], axis=1))
        ahead = jnp.zeros((rows, rc), f32)
        for l in range(blocks):
            if l < blocks - 1:
                ahead = jnp.where(row_block == l + 1, forward_rows(own, l), ahead)
            else:
                ahead = jnp.where(row_block == 0, forward_rows(other, l), ahead)
        ahead = pltpu.roll(ahead, rows - 2, 0)

        surf = []
        edge = peer_in[par, 0, rows : rows + 8, :]
        for p in range(2):
            prod = surface_ref[...] * to_col(edge[p : p + 1])
            surf.append(
                [
                    jnp.sum(prod[l * ch : (l + 1) * ch], axis=0, keepdims=True)
                    for l in range(blocks)
                ]
            )
        surf = jnp.concatenate(
            [surf[p][l] for l in range(blocks) for p in range(2)], axis=0
        )

        @pl.when(has_below)
        def _():
            wait(grid.at[par, :, pl.ds(0, ch), :], sem_up_recv.at[par])

        @pl.when(has_above)
        def _():
            wait(grid.at[par, :, pl.ds(0, ch), :], sem_down_recv.at[par])

        bound = jnp.zeros((8, width), f32)
        for k in range(sectors):
            bound = bound + peer_in[par, k, rows : rows + 8, :]
        before = peer_in[par, lax.rem(me + sectors - 1, sectors), rows : rows + 8, :]
        after = peer_in[par, lax.rem(me + 1, sectors), rows : rows + 8, :]
        lane = lax.broadcasted_iota(jnp.int32, (1, nr), 1)
        for p in range(2):
            gh, gl = split(grid[par, p])
            r = lax.dot_general(mix_split[...], gh, NN, preferred_element_type=f32)
            q = lax.dot_general(mix_split[0:nc, :], gl, NN, preferred_element_type=f32)
            coupled = r[:nc] + r[nc:] + q
            left_row = jnp.where(me == 0, bound[4 + p : 5 + p], before[2 + p : 3 + p])
            right_row = jnp.where(me == sectors - 1, 0.0, after[p : p + 1])
            left_col = to_col(left_row)
            right_col = to_col(right_row)
            x = grid[par, p, ch : ch + nc, :]
            left = jnp.where(lane == 0, left_col, pltpu.roll(x, 1, 1))
            right = jnp.where(lane == nr - 1, right_col, pltpu.roll(x, nr - 1, 1))
            image = diag_ref[...] * x - kinetic_scale * (left + right) + strength * coupled
            value = (factor if p == 1 else -factor) * image
            acc = outer_out[1 - p] + value
            outer_out[1 - p] = acc
            grid[nxt, 1 - p, ch : ch + nc, :] = jnp.where(last, acc, value)

        wait(part_in.at[par, pl.ds(0, sectors - 1)], sem_b_recv.at[par])

        @pl.when(has_below)
        def _():
            wait(below_in.at[par], sem_y_recv.at[par])

        near = part_in[par, 0]
        far = below_in[par, 0]
        for k in range(1, sectors):
            near = near + part_in[par, k]
            far = far + below_in[par, k]
        behind = jnp.where(row_block == 0, far, near)
        image = live_ref[...] * (
            energy_ref[...] * c + strength * (ahead + behind) - kinetic_scale * surf
        )
        even = lax.rem(lax.broadcasted_iota(jnp.int32, (rows, 1), 0), 2) == 0
        value = factor * jnp.where(
            even, pltpu.roll(image, rows - 1, 0), -pltpu.roll(image, 1, 0)
        )
        acc = inner_out[...] + value
        inner_out[...] = acc
        term[...] = jnp.where(last, acc, value)

        wait(peer_in.at[par, pl.ds(0, sectors - 1)], sem_a_send)
        wait(part_in.at[par, pl.ds(0, sectors - 1)], sem_b_send)

        @pl.when(has_below)
        def _():
            wait(above_in.at[par], sem_z_send)
            down.wait_send()

        @pl.when(has_above)
        def _():
            wait(below_in.at[par], sem_y_send)
            up.wait_send()

        return carry

    lax.fori_loop(0, STEPS * ORDER, apply, 0)


def local(
    planes,
    sectors,
    inner_state,
    outer_state,
    energies,
    dipole,
    surface,
    thresholds,
    coupling_coef,
    coupling_pattern,
    block_sizes,
    field_strength,
):
    blocks, rc, total = dipole.shape
    ch = coupling_coef.shape[1]
    nc, nr = outer_state.shape[1:]
    rows = 2 * blocks
    width = max(rc, -(-nc // 128) * 128)
    row_index = lax.axis_index("outer") * rc + jnp.arange(rc, dtype=jnp.int32)
    live = (row_index[None, :] < block_sizes[:, None]).astype(f32)
    coupling = coupling_coef * coupling_pattern.astype(f32)
    below = lax.ppermute(coupling[blocks - 1], "inner", [(i, i + 1) for i in range(planes - 1)])
    mix = jnp.zeros((nc, nc + 2 * ch), f32)
    for l in range(blocks):
        source = below if l == 0 else coupling[l - 1]
        mix = mix.at[l * ch : (l + 1) * ch, l * ch : (l + 1) * ch].set(source.T)
        mix = mix.at[l * ch : (l + 1) * ch, (l + 2) * ch : (l + 3) * ch].set(coupling[l])
    diag = (thresholds + 2.0 * kinetic_scale)[:, None]
    vmem = pl.BlockSpec(memory_space=pltpu.VMEM)
    dma = pltpu.SemaphoreType.DMA
    inner_final, outer_final = pl.pallas_call(
        functools.partial(kernel, planes, sectors, ch),
        out_shape=(
            jax.ShapeDtypeStruct((rows, rc), f32),
            jax.ShapeDtypeStruct((2, nc, nr), f32),
        ),
        in_specs=[vmem] * 8 + [pl.BlockSpec(memory_space=pltpu.SMEM)],
        out_specs=(vmem, vmem),
        scratch_shapes=[
            pltpu.VMEM((blocks * rc, total), bf16),
            pltpu.VMEM((blocks * rc, total), bf16),
            pltpu.VMEM((2 * nc, nc + 2 * ch), bf16),
            pltpu.VMEM((2, 2, nc + 2 * ch, nr), f32),
            pltpu.VMEM((rows, rc), f32),
            pltpu.VMEM((2, sectors, rows + 8, width), f32),
            pltpu.VMEM((2, sectors, rows, rc), f32),
            pltpu.VMEM((sectors, rows, rc), f32),
            pltpu.VMEM((2, sectors, rows, rc), f32),
            pltpu.VMEM((2, sectors, rows, rc), f32),
            pltpu.VMEM((8, 128), f32),
            dma(()), dma((2,)), dma(()), dma((2,)),
            dma(()), dma((2,)), dma(()), dma((2,)),
            dma(()), dma((2,)), dma(()), dma((2,)),
        ],
        compiler_params=pltpu.CompilerParams(
            has_side_effects=True, vmem_limit_bytes=56 * 1024 * 1024
        ),
    )(
        inner_state.transpose(1, 0, 2).reshape(rows, rc),
        outer_state,
        jnp.repeat(live, 2, axis=0),
        jnp.repeat(energies, 2, axis=0),
        dipole.reshape(blocks * rc, total),
        surface.reshape(nc, rc),
        diag,
        mix,
        field_strength,
    )
    return inner_final.reshape(blocks, 2, rc).transpose(1, 0, 2), outer_final


def solution(mesh):
    placed = (
        P(None, "inner", "outer"),
        P(None, "inner", "outer"),
        P("inner", "outer"),
        P("inner", "outer", None),
        P("inner", None, "outer"),
        P("inner"),
        P("inner", None, None),
        P("inner", None, None),
        P("inner"),
        P(),
    )
    return jax.shard_map(
        functools.partial(local, mesh.shape["inner"], mesh.shape["outer"]),
        mesh=mesh,
        in_specs=placed,
        out_specs=(P(None, "inner", "outer"), P(None, "inner", "outer")),
        check_vma=False,
    )
```

```python
import functools

import jax
import jax.numpy as jnp
from jax import lax
from jax.experimental import pallas as pl
from jax.experimental.pallas import tpu as pltpu
from jax.sharding import PartitionSpec as P

STEPS = 2
ORDER = 4

kinetic_scale = 3.125
time_step = 0.1

MESH = pl.DeviceIdType.MESH
f32 = jnp.float32
bf16 = jnp.bfloat16
NT = (((1,), (1,)), ((), ()))
NN = (((1,), (0,)), ((), ()))


def split(x):
    high = x.astype(bf16)
    return high, (x - high.astype(f32)).astype(bf16)


def kernel(
    planes,
    sectors,
    ch,
    inner_ref,
    outer_ref,
    energy_ref,
    dipole_ref,
    surface_ref,
    threshold_ref,
    coef_ref,
    pattern_ref,
    size_ref,
    field_ref,
    inner_out,
    outer_out,
    dip_hi,
    dip_lo,
    mix_split,
    grid,
    term,
    peer_in,
    above_in,
    part_out,
    part_in,
    below_in,
    pairs,
    dip_full,
    live_ref,
    energy_rows,
    total_inner,
    diag_ref,
    sem_load,
    sem_g_send,
    sem_g_recv,
    sem_a_send,
    sem_a_recv,
    sem_z_send,
    sem_z_recv,
    sem_b_send,
    sem_b_recv,
    sem_y_send,
    sem_y_recv,
    sem_up_send,
    sem_up_recv,
    sem_down_send,
    sem_down_recv,
):
    z = lax.axis_index("inner")
    me = lax.axis_index("outer")
    blocks, rc = energy_ref.shape
    rows = 2 * blocks
    nc, nr = outer_ref.shape[1:]
    total = rc * sectors
    width = peer_in.shape[3]
    has_below = z > 0
    has_above = z < planes - 1

    @pl.when(z == 0)
    def _():
        below_in[...] = jnp.zeros_like(below_in)
        grid[:, :, 0:ch, :] = jnp.zeros((2, 2, ch, nr), f32)

    @pl.when(z == planes - 1)
    def _():
        above_in[...] = jnp.zeros_like(above_in)
        grid[:, :, ch + nc : 2 * ch + nc, :] = jnp.zeros((2, 2, ch, nr), f32)

    loads = [
        pltpu.make_async_copy(
            dipole_ref.at[pl.ds(l * rc, rc)], dip_full.at[pl.ds(l * rc, rc)], sem_load.at[l]
        )
        for l in range(blocks)
    ]
    for load in loads:
        load.start()

    for p in (1, 0):
        x = outer_ref[p]
        grid[0, p, ch : ch + nc, :] = x
        outer_out[p] = x

    def channel_copies(slot, p):
        up = pltpu.make_async_remote_copy(
            src_ref=grid.at[slot, p, pl.ds(nc, ch), :],
            dst_ref=grid.at[slot, p, pl.ds(0, ch), :],
            send_sem=sem_up_send.at[p],
            recv_sem=sem_up_recv.at[slot, p],
            device_id={"inner": z + 1, "outer": me},
            device_id_type=MESH,
        )
        down = pltpu.make_async_remote_copy(
            src_ref=grid.at[slot, p, pl.ds(ch, ch), :],
            dst_ref=grid.at[slot, p, pl.ds(ch + nc, ch), :],
            send_sem=sem_down_send.at[p],
            recv_sem=sem_down_recv.at[slot, p],
            device_id={"inner": z - 1, "outer": me},
            device_id_type=MESH,
        )
        return up, down

    side = pairs.shape[1]
    for l in range(blocks + 1):
        pairs[l, ch:side, :] = jnp.zeros((side - ch, side), f32)
    for l in range(blocks):
        pairs[l + 1, 0:ch, :] = jnp.zeros((ch, side), f32)
        pairs[l + 1, 0:ch, 0:ch] = coef_ref[l] * pattern_ref[l].astype(f32)

    @pl.when(z == 0)
    def _():
        pairs[0, 0:ch, :] = jnp.zeros((ch, side), f32)

    share = pltpu.make_async_remote_copy(
        src_ref=pairs.at[blocks, pl.ds(0, ch), :],
        dst_ref=pairs.at[0, pl.ds(0, ch), :],
        send_sem=sem_g_send,
        recv_sem=sem_g_recv,
        device_id={"inner": z + 1, "outer": me},
        device_id_type=MESH,
    )

    @pl.when(has_above)
    def _():
        share.start()
        for p in (1, 0):
            channel_copies(0, p)[0].start()

    @pl.when(has_below)
    def _():
        for p in (1, 0):
            channel_copies(0, p)[1].start()

    order_of = [(l, p) for l in range(blocks) for p in range(2)]
    position = me * rc + lax.broadcasted_iota(jnp.int32, (1, rc), 1)
    live_ref[...] = jnp.concatenate(
        [jnp.where(position < size_ref[l], 1.0, 0.0) for l, p in order_of], axis=0
    )
    energy_rows[...] = jnp.concatenate([energy_ref[l : l + 1, :] for l, p in order_of], axis=0)
    term[...] = live_ref[...] * jnp.concatenate(
        [inner_ref[p, l : l + 1, :] for l, p in order_of], axis=0
    )
    total_inner[...] = term[...]

    eye = lax.broadcasted_iota(jnp.int32, (nc, width), 0) == lax.broadcasted_iota(
        jnp.int32, (nc, width), 1
    )

    def to_row(col):
        return jnp.sum(jnp.where(eye, col, 0.0), axis=0, keepdims=True)

    def to_col(row):
        return jnp.sum(jnp.where(eye, row, 0.0), axis=1, keepdims=True)

    def wait(ref, sem):
        pltpu.make_async_copy(ref, ref, sem).wait()

    small = lax.broadcasted_iota(jnp.int32, (nc, nc), 0) == lax.broadcasted_iota(
        jnp.int32, (nc, nc), 1
    )
    diag_ref[...] = 2.0 * kinetic_scale + jnp.sum(
        jnp.where(small, threshold_ref[...], 0.0), axis=1, keepdims=True
    )

    def split_rows(i, carry):
        at = pl.ds(pl.multiple_of(i * 16, 16), 16)
        high, low = split(dip_full[at, :])
        dip_hi[at, :] = high
        dip_lo[at, :] = low
        return carry

    for l in range(blocks):
        loads[l].wait()
        lax.fori_loop(l * (rc // 16), (l + 1) * (rc // 16), split_rows, 0)

    @pl.when(has_below)
    def _():
        share.wait_recv()

    @pl.when(has_above)
    def _():
        share.wait_send()

    reach = -(-(nc + 2 * ch) // 128) * 128
    fill = jnp.zeros((ch, reach - side), f32)
    mixed_rows = []
    for l in range(blocks):
        upward = jnp.concatenate([pairs[l + 1, 0:ch, :], fill], axis=1)
        downward = jnp.concatenate([pairs[l].T[0:ch], fill], axis=1)
        upward = pltpu.roll(upward, (l + 2) * ch, 1)
        if l:
            downward = pltpu.roll(downward, l * ch, 1)
        mixed_rows.append((upward + downward)[:, 0 : nc + 2 * ch])
    mh, ml = split(jnp.concatenate(mixed_rows, axis=0))
    mix_split[0:nc, :] = mh
    mix_split[nc : 2 * nc, :] = ml

    def apply(t, carry):
        par = lax.rem(t, 2)
        nxt = 1 - par
        order = lax.rem(t, ORDER)
        strength = field_ref[lax.div(t, ORDER)]
        factor = time_step / (order + 1).astype(f32)
        last = order == ORDER - 1

        c = term[...]
        peer_in[par, me, 0:rows, 0:rc] = c
        edge_rows = []
        for p in range(2):
            edge_rows.append(to_row(grid[par, p, ch : ch + nc, 0:1]))
        for p in range(2):
            edge_rows.append(to_row(grid[par, p, ch : ch + nc, nr - 1 : nr]))
        for p in range(2):
            spread = jnp.concatenate(
                [
                    jnp.broadcast_to(c[2 * l + p : 2 * l + p + 1], (ch, rc))
                    for l in range(blocks)
                ],
                axis=0,
            )
            edge_rows.append(
                to_row(jnp.sum(surface_ref[...] * spread, axis=1, keepdims=True))
            )
        edge_rows.append(jnp.zeros((2, width), f32))
        peer_in[par, me, rows : rows + 8, :] = jnp.concatenate(edge_rows, axis=0)

        @pl.when(has_below)
        def _():
            def send_z(s, k):
                to = lax.rem(me + s, sectors)
                pltpu.make_async_remote_copy(
                    src_ref=peer_in.at[par, me, pl.ds(0, 2), pl.ds(0, rc)],
                    dst_ref=above_in.at[par, me, pl.ds(0, 2)],
                    send_sem=sem_z_send,
                    recv_sem=sem_z_recv.at[par],
                    device_id={"inner": z - 1, "outer": to},
                    device_id_type=MESH,
                ).start()
                return k

            lax.fori_loop(0, sectors, send_z, 0)

        def send_a(s, k):
            to = lax.rem(me + s, sectors)
            pltpu.make_async_remote_copy(
                src_ref=peer_in.at[par, me],
                dst_ref=peer_in.at[par, me],
                send_sem=sem_a_send,
                recv_sem=sem_a_recv.at[par],
                device_id={"inner": z, "outer": to},
                device_id_type=MESH,
            ).start()
            return k

        lax.fori_loop(1, sectors, send_a, 0)

        row_block = lax.broadcasted_iota(jnp.int32, (rows, 1), 0) // 2
        ch_, cl_ = split(c)
        both = jnp.concatenate([ch_, cl_], axis=0)
        back = jnp.zeros((rows, total), f32)
        for l in range(blocks):
            at = pl.ds(l * rc, rc)
            r = lax.dot_general(both, dip_hi[at, :], NN, preferred_element_type=f32)
            q = lax.dot_general(ch_, dip_lo[at, :], NN, preferred_element_type=f32)
            back = jnp.where(row_block == l, r[:rows] + r[rows:] + q, back)
        back = pltpu.roll(back, 2, 0)
        for k in range(sectors):
            part_out[k] = back[:, k * rc : (k + 1) * rc]
        part_in[par, me] = part_out[me]

        @pl.when(has_above)
        def _():
            def send_y(s, k):
                to = lax.rem(me + s, sectors)
                pltpu.make_async_remote_copy(
                    src_ref=part_out.at[to, pl.ds(0, 2)],
                    dst_ref=below_in.at[par, me, pl.ds(0, 2)],
                    send_sem=sem_y_send,
                    recv_sem=sem_y_recv.at[par],
                    device_id={"inner": z + 1, "outer": to},
                    device_id_type=MESH,
                ).start()
                return k

            lax.fori_loop(0, sectors, send_y, 0)

        def send_b(s, k):
            to = lax.rem(me + s, sectors)
            pltpu.make_async_remote_copy(
                src_ref=part_out.at[to],
                dst_ref=part_in.at[par, me],
                send_sem=sem_b_send,
                recv_sem=sem_b_recv.at[par],
                device_id={"inner": z, "outer": to},
                device_id_type=MESH,
            ).start()
            return k

        lax.fori_loop(1, sectors, send_b, 0)

        wait(peer_in.at[par, pl.ds(0, sectors - 1)], sem_a_recv.at[par])

        @pl.when(has_above)
        def _():
            wait(above_in.at[par, :, pl.ds(0, 2)], sem_z_recv.at[par])

        def forward_rows(values, l):
            vh, vl = values
            at = pl.ds(l * rc, rc)
            r = lax.dot_general(
                jnp.concatenate([vh, vl], axis=0), dip_hi[at, :], NT, preferred_element_type=f32
            )
            q = lax.dot_general(vh, dip_lo[at, :], NT, preferred_element_type=f32)
            return r[:rows] + r[rows:] + q

        own = split(
            jnp.concatenate([peer_in[par, k, 0:rows, 0:rc] for k in range(sectors)], axis=1)
        )
        other = split(jnp.concatenate([above_in[par, k] for k in range(sectors)], axis=1))
        ahead = jnp.zeros((rows, rc), f32)
        for l in range(blocks):
            if l < blocks - 1:
                ahead = jnp.where(row_block == l + 1, forward_rows(own, l), ahead)
            else:
                ahead = jnp.where(row_block == 0, forward_rows(other, l), ahead)
        ahead = pltpu.roll(ahead, rows - 2, 0)

        surf = []
        edge = peer_in[par, 0, rows : rows + 8, :]
        for p in range(2):
            prod = surface_ref[...] * to_col(edge[p : p + 1])
            surf.append(
                [
                    jnp.sum(prod[l * ch : (l + 1) * ch], axis=0, keepdims=True)
                    for l in range(blocks)
                ]
            )
        surf = jnp.concatenate(
            [surf[p][l] for l in range(blocks) for p in range(2)], axis=0
        )

        bound = jnp.zeros((8, width), f32)
        for k in range(sectors):
            bound = bound + peer_in[par, k, rows : rows + 8, :]
        before = peer_in[par, lax.rem(me + sectors - 1, sectors), rows : rows + 8, :]
        after = peer_in[par, lax.rem(me + 1, sectors), rows : rows + 8, :]
        lane = lax.broadcasted_iota(jnp.int32, (1, nr), 1)
        for p in (1, 0):
            up, down = channel_copies(par, p)

            @pl.when(has_below)
            def _():
                up.wait_recv()

            @pl.when(has_above)
            def _():
                down.wait_recv()

            gh, gl = split(grid[par, p])
            r = lax.dot_general(mix_split[...], gh, NN, preferred_element_type=f32)
            q = lax.dot_general(mix_split[0:nc, :], gl, NN, preferred_element_type=f32)
            coupled = r[:nc] + r[nc:] + q
            left_row = jnp.where(me == 0, bound[4 + p : 5 + p], before[2 + p : 3 + p])
            right_row = jnp.where(me == sectors - 1, 0.0, after[p : p + 1])
            left_col = to_col(left_row)
            right_col = to_col(right_row)
            x = grid[par, p, ch : ch + nc, :]
            left = jnp.where(lane == 0, left_col, pltpu.roll(x, 1, 1))
            right = jnp.where(lane == nr - 1, right_col, pltpu.roll(x, nr - 1, 1))
            image = diag_ref[...] * x - kinetic_scale * (left + right) + strength * coupled
            value = (factor if p == 1 else -factor) * image
            acc = outer_out[1 - p] + value
            outer_out[1 - p] = acc
            grid[nxt, 1 - p, ch : ch + nc, :] = jnp.where(last, acc, value)
            new_up, new_down = channel_copies(nxt, 1 - p)
            up_old, down_old = channel_copies(par, 1 - p)

            @pl.when(has_above)
            def _():
                up_old.wait_send()

            @pl.when(has_below)
            def _():
                down_old.wait_send()

            @pl.when(jnp.logical_and(has_above, t < STEPS * ORDER - 1))
            def _():
                new_up.start()

            @pl.when(jnp.logical_and(has_below, t < STEPS * ORDER - 1))
            def _():
                new_down.start()


        wait(part_in.at[par, pl.ds(0, sectors - 1)], sem_b_recv.at[par])

        @pl.when(has_below)
        def _():
            wait(below_in.at[par, :, pl.ds(0, 2)], sem_y_recv.at[par])

        near = part_in[par, 0]
        far = below_in[par, 0]
        for k in range(1, sectors):
            near = near + part_in[par, k]
            far = far + below_in[par, k]
        behind = jnp.where(row_block == 0, far, near)
        image = live_ref[...] * (
            energy_rows[...] * c + strength * (ahead + behind) - kinetic_scale * surf
        )
        even = lax.rem(lax.broadcasted_iota(jnp.int32, (rows, 1), 0), 2) == 0
        value = factor * jnp.where(
            even, pltpu.roll(image, rows - 1, 0), -pltpu.roll(image, 1, 0)
        )
        acc = total_inner[...] + value
        total_inner[...] = acc
        term[...] = jnp.where(last, acc, value)

        wait(peer_in.at[par, pl.ds(0, sectors - 1)], sem_a_send)
        wait(part_in.at[par, pl.ds(0, sectors - 1)], sem_b_send)

        @pl.when(has_below)
        def _():
            wait(above_in.at[par, :, pl.ds(0, 2)], sem_z_send)

        @pl.when(has_above)
        def _():
            wait(below_in.at[par, :, pl.ds(0, 2)], sem_y_send)

        return carry

    lax.fori_loop(0, STEPS * ORDER, apply, 0)
    final = total_inner[...]
    for p in range(2):
        inner_out[p] = jnp.concatenate(
            [final[2 * l + p : 2 * l + p + 1] for l in range(blocks)], axis=0
        )


def local(
    planes,
    sectors,
    inner_state,
    outer_state,
    energies,
    dipole,
    surface,
    thresholds,
    coupling_coef,
    coupling_pattern,
    block_sizes,
    field_strength,
):
    blocks, rc, total = dipole.shape
    ch = coupling_coef.shape[1]
    nc, nr = outer_state.shape[1:]
    rows = 2 * blocks
    width = max(rc, -(-nc // 128) * 128)
    vmem = pl.BlockSpec(memory_space=pltpu.VMEM)
    dma = pltpu.SemaphoreType.DMA
    smem = pl.BlockSpec(memory_space=pltpu.SMEM)
    side = -(-ch // 128) * 128
    return pl.pallas_call(
        functools.partial(kernel, planes, sectors, ch),
        out_shape=(
            jax.ShapeDtypeStruct((2, blocks, rc), f32),
            jax.ShapeDtypeStruct((2, nc, nr), f32),
        ),
        in_specs=[vmem] * 3
        + [pl.BlockSpec(memory_space=pltpu.HBM)]
        + [vmem] * 4
        + [smem] * 2,
        out_specs=(vmem, vmem),
        scratch_shapes=[
            pltpu.VMEM((blocks * rc, total), bf16),
            pltpu.VMEM((blocks * rc, total), bf16),
            pltpu.VMEM((2 * nc, nc + 2 * ch), bf16),
            pltpu.VMEM((2, 2, nc + 2 * ch, nr), f32),
            pltpu.VMEM((rows, rc), f32),
            pltpu.VMEM((2, sectors, rows + 8, width), f32),
            pltpu.VMEM((2, sectors, rows, rc), f32),
            pltpu.VMEM((sectors, rows, rc), f32),
            pltpu.VMEM((2, sectors, rows, rc), f32),
            pltpu.VMEM((2, sectors, rows, rc), f32),
            pltpu.VMEM((blocks + 1, side, side), f32),
            pltpu.VMEM((blocks * rc, total), f32),
            pltpu.VMEM((rows, rc), f32),
            pltpu.VMEM((rows, rc), f32),
            pltpu.VMEM((rows, rc), f32),
            pltpu.VMEM((nc, 1), f32),
            dma((blocks,)), dma(()), dma(()),
            dma(()), dma((2,)), dma(()), dma((2,)),
            dma(()), dma((2,)), dma(()), dma((2,)),
            dma((2,)), dma((2, 2)), dma((2,)), dma((2, 2)),
        ],
        compiler_params=pltpu.CompilerParams(
            has_side_effects=True, vmem_limit_bytes=56 * 1024 * 1024
        ),
    )(
        inner_state,
        outer_state,
        energies,
        dipole.reshape(blocks * rc, total),
        surface.reshape(nc, rc),
        thresholds.reshape(1, nc),
        coupling_coef,
        coupling_pattern,
        block_sizes,
        field_strength,
    )


def solution(mesh):
    placed = (
        P(None, "inner", "outer"),
        P(None, "inner", "outer"),
        P("inner", "outer"),
        P("inner", "outer", None),
        P("inner", None, "outer"),
        P("inner"),
        P("inner", None, None),
        P("inner", None, None),
        P("inner"),
        P(),
    )
    return jax.shard_map(
        functools.partial(local, mesh.shape["inner"], mesh.shape["outer"]),
        mesh=mesh,
        in_specs=placed,
        out_specs=(P(None, "inner", "outer"), P(None, "inner", "outer")),
        check_vma=False,
    )
```

```python
import functools

import jax
import jax.numpy as jnp
from jax import lax
from jax.experimental import pallas as pl
from jax.experimental.pallas import tpu as pltpu
from jax.sharding import PartitionSpec as P

STEPS = 2
ORDER = 4

kinetic_scale = 3.125
time_step = 0.1

MESH = pl.DeviceIdType.MESH
f32 = jnp.float32
bf16 = jnp.bfloat16
NT = (((1,), (1,)), ((), ()))
NN = (((1,), (0,)), ((), ()))


def split(x):
    high = x.astype(bf16)
    return high, (x - high.astype(f32)).astype(bf16)


def kernel(
    planes,
    sectors,
    ch,
    inner_ref,
    outer_ref,
    energy_ref,
    dipole_ref,
    surface_ref,
    threshold_ref,
    coef_ref,
    pattern_ref,
    size_ref,
    field_ref,
    inner_out,
    outer_out,
    dip_hi,
    dip_lo,
    mix_split,
    grid,
    term,
    peer_in,
    above_in,
    part_out,
    part_in,
    below_in,
    pairs,
    dip_full,
    live_ref,
    energy_rows,
    total_inner,
    diag_ref,
    edge_in,
    sem_e_send,
    sem_e_recv,
    sem_load,
    sem_g_send,
    sem_g_recv,
    sem_a_send,
    sem_a_recv,
    sem_z_send,
    sem_z_recv,
    sem_b_send,
    sem_b_recv,
    sem_y_send,
    sem_y_recv,
    sem_up_send,
    sem_up_recv,
    sem_down_send,
    sem_down_recv,
):
    z = lax.axis_index("inner")
    me = lax.axis_index("outer")
    blocks, rc = energy_ref.shape
    rows = 2 * blocks
    nc, nr = outer_ref.shape[1:]
    total = rc * sectors
    width = edge_in.shape[3]
    has_below = z > 0
    has_above = z < planes - 1

    @pl.when(z == 0)
    def _():
        below_in[...] = jnp.zeros_like(below_in)
        grid[:, :, 0:ch, :] = jnp.zeros((2, 2, ch, nr), f32)

    @pl.when(z == planes - 1)
    def _():
        above_in[...] = jnp.zeros_like(above_in)
        grid[:, :, ch + nc : 2 * ch + nc, :] = jnp.zeros((2, 2, ch, nr), f32)

    loads = [
        pltpu.make_async_copy(
            dipole_ref.at[pl.ds(l * rc, rc)], dip_full.at[pl.ds(l * rc, rc)], sem_load.at[l]
        )
        for l in range(blocks)
    ]
    for load in loads:
        load.start()

    for p in (1, 0):
        x = outer_ref[p]
        grid[0, p, ch : ch + nc, :] = x
        outer_out[p] = x

    def channel_copies(slot, p):
        up = pltpu.make_async_remote_copy(
            src_ref=grid.at[slot, p, pl.ds(nc, ch), :],
            dst_ref=grid.at[slot, p, pl.ds(0, ch), :],
            send_sem=sem_up_send.at[p],
            recv_sem=sem_up_recv.at[slot, p],
            device_id={"inner": z + 1, "outer": me},
            device_id_type=MESH,
        )
        down = pltpu.make_async_remote_copy(
            src_ref=grid.at[slot, p, pl.ds(ch, ch), :],
            dst_ref=grid.at[slot, p, pl.ds(ch + nc, ch), :],
            send_sem=sem_down_send.at[p],
            recv_sem=sem_down_recv.at[slot, p],
            device_id={"inner": z - 1, "outer": me},
            device_id_type=MESH,
        )
        return up, down

    side = pairs.shape[1]
    for l in range(blocks + 1):
        pairs[l, ch:side, :] = jnp.zeros((side - ch, side), f32)
    for l in range(blocks):
        pairs[l + 1, 0:ch, :] = jnp.zeros((ch, side), f32)
        pairs[l + 1, 0:ch, 0:ch] = coef_ref[l] * pattern_ref[l].astype(f32)

    @pl.when(z == 0)
    def _():
        pairs[0, 0:ch, :] = jnp.zeros((ch, side), f32)

    share = pltpu.make_async_remote_copy(
        src_ref=pairs.at[blocks, pl.ds(0, ch), :],
        dst_ref=pairs.at[0, pl.ds(0, ch), :],
        send_sem=sem_g_send,
        recv_sem=sem_g_recv,
        device_id={"inner": z + 1, "outer": me},
        device_id_type=MESH,
    )

    @pl.when(has_above)
    def _():
        share.start()
        for p in (1, 0):
            channel_copies(0, p)[0].start()

    @pl.when(has_below)
    def _():
        for p in (1, 0):
            channel_copies(0, p)[1].start()

    order_of = [(l, p) for l in range(blocks) for p in range(2)]
    position = me * rc + lax.broadcasted_iota(jnp.int32, (1, rc), 1)
    live_ref[...] = jnp.concatenate(
        [jnp.where(position < size_ref[l], 1.0, 0.0) for l, p in order_of], axis=0
    )
    energy_rows[...] = jnp.concatenate([energy_ref[l : l + 1, :] for l, p in order_of], axis=0)
    term[...] = live_ref[...] * jnp.concatenate(
        [inner_ref[p, l : l + 1, :] for l, p in order_of], axis=0
    )
    total_inner[...] = term[...]

    eye = lax.broadcasted_iota(jnp.int32, (nc, width), 0) == lax.broadcasted_iota(
        jnp.int32, (nc, width), 1
    )

    def to_row(col):
        return jnp.sum(jnp.where(eye, col, 0.0), axis=0, keepdims=True)

    def to_col(row):
        return jnp.sum(jnp.where(eye, row, 0.0), axis=1, keepdims=True)

    def wait(ref, sem):
        pltpu.make_async_copy(ref, ref, sem).wait()

    small = lax.broadcasted_iota(jnp.int32, (nc, nc), 0) == lax.broadcasted_iota(
        jnp.int32, (nc, nc), 1
    )
    diag_ref[...] = 2.0 * kinetic_scale + jnp.sum(
        jnp.where(small, threshold_ref[...], 0.0), axis=1, keepdims=True
    )

    def split_rows(i, carry):
        at = pl.ds(pl.multiple_of(i * 16, 16), 16)
        high, low = split(dip_full[at, :])
        dip_hi[at, :] = high
        dip_lo[at, :] = low
        return carry

    for l in range(blocks):
        loads[l].wait()
        lax.fori_loop(l * (rc // 16), (l + 1) * (rc // 16), split_rows, 0)

    @pl.when(has_below)
    def _():
        share.wait_recv()

    @pl.when(has_above)
    def _():
        share.wait_send()

    reach = -(-(nc + 2 * ch) // 128) * 128
    fill = jnp.zeros((ch, reach - side), f32)
    mixed_rows = []
    for l in range(blocks):
        upward = jnp.concatenate([pairs[l + 1, 0:ch, :], fill], axis=1)
        downward = jnp.concatenate([pairs[l].T[0:ch], fill], axis=1)
        upward = pltpu.roll(upward, (l + 2) * ch, 1)
        if l:
            downward = pltpu.roll(downward, l * ch, 1)
        mixed_rows.append((upward + downward)[:, 0 : nc + 2 * ch])
    mh, ml = split(jnp.concatenate(mixed_rows, axis=0))
    mix_split[0:nc, :] = mh
    mix_split[nc : 2 * nc, :] = ml

    def apply(t, carry):
        par = lax.rem(t, 2)
        nxt = 1 - par
        order = lax.rem(t, ORDER)
        strength = field_ref[lax.div(t, ORDER)]
        factor = time_step / (order + 1).astype(f32)
        last = order == ORDER - 1

        c = term[...]
        peer_in[par, me, 0:rows, 0:rc] = c
        def send_a(s, k):
            to = lax.rem(me + s, sectors)
            pltpu.make_async_remote_copy(
                src_ref=peer_in.at[par, me],
                dst_ref=peer_in.at[par, me],
                send_sem=sem_a_send,
                recv_sem=sem_a_recv.at[par],
                device_id={"inner": z, "outer": to},
                device_id_type=MESH,
            ).start()
            return k

        lax.fori_loop(1, sectors, send_a, 0)

        @pl.when(has_below)
        def _():
            def send_z(s, k):
                to = lax.rem(me + s, sectors)
                pltpu.make_async_remote_copy(
                    src_ref=peer_in.at[par, me, pl.ds(0, 2), pl.ds(0, rc)],
                    dst_ref=above_in.at[par, me, pl.ds(0, 2)],
                    send_sem=sem_z_send,
                    recv_sem=sem_z_recv.at[par],
                    device_id={"inner": z - 1, "outer": to},
                    device_id_type=MESH,
                ).start()
                return k

            lax.fori_loop(0, sectors, send_z, 0)

        edge_rows = []
        for p in range(2):
            edge_rows.append(to_row(grid[par, p, ch : ch + nc, 0:1]))
        for p in range(2):
            edge_rows.append(to_row(grid[par, p, ch : ch + nc, nr - 1 : nr]))
        for p in range(2):
            spread = jnp.concatenate(
                [
                    jnp.broadcast_to(c[2 * l + p : 2 * l + p + 1], (ch, rc))
                    for l in range(blocks)
                ],
                axis=0,
            )
            edge_rows.append(
                to_row(jnp.sum(surface_ref[...] * spread, axis=1, keepdims=True))
            )
        edge_rows.append(jnp.zeros((2, width), f32))
        edge_in[par, me] = jnp.concatenate(edge_rows, axis=0)

        def edge_copy(s):
            to = lax.rem(me + s, sectors)
            need = (s == 1) | (s == sectors - 1) | (to == 0) | (me == 0)
            out = pltpu.make_async_remote_copy(
                src_ref=edge_in.at[par, me],
                dst_ref=edge_in.at[par, me],
                send_sem=sem_e_send.at[to],
                recv_sem=sem_e_recv.at[par, me],
                device_id={"inner": z, "outer": to},
                device_id_type=MESH,
            )
            return need, to, out

        def send_e(s, k):
            need, to, out = edge_copy(s)

            @pl.when(need)
            def _():
                out.start()

            return k

        lax.fori_loop(1, sectors, send_e, 0)

        row_block = lax.broadcasted_iota(jnp.int32, (rows, 1), 0) // 2
        ch_, cl_ = split(c)
        both = jnp.concatenate([ch_, cl_], axis=0)
        back = jnp.zeros((rows, total), f32)
        for l in range(blocks):
            at = pl.ds(l * rc, rc)
            r = lax.dot_general(both, dip_hi[at, :], NN, preferred_element_type=f32)
            q = lax.dot_general(ch_, dip_lo[at, :], NN, preferred_element_type=f32)
            back = jnp.where(row_block == l, r[:rows] + r[rows:] + q, back)
        back = pltpu.roll(back, 2, 0)
        for k in range(sectors):
            part_out[k] = back[:, k * rc : (k + 1) * rc]
        part_in[par, me] = part_out[me]

        @pl.when(has_above)
        def _():
            def send_y(s, k):
                to = lax.rem(me + s, sectors)
                pltpu.make_async_remote_copy(
                    src_ref=part_out.at[to, pl.ds(0, 2)],
                    dst_ref=below_in.at[par, me, pl.ds(0, 2)],
                    send_sem=sem_y_send,
                    recv_sem=sem_y_recv.at[par],
                    device_id={"inner": z + 1, "outer": to},
                    device_id_type=MESH,
                ).start()
                return k

            lax.fori_loop(0, sectors, send_y, 0)

        def send_b(s, k):
            to = lax.rem(me + s, sectors)
            pltpu.make_async_remote_copy(
                src_ref=part_out.at[to],
                dst_ref=part_in.at[par, me],
                send_sem=sem_b_send,
                recv_sem=sem_b_recv.at[par],
                device_id={"inner": z, "outer": to},
                device_id_type=MESH,
            ).start()
            return k

        lax.fori_loop(1, sectors, send_b, 0)

        wait(peer_in.at[par, pl.ds(0, sectors - 1)], sem_a_recv.at[par])

        def forward_rows(values, l):
            vh, vl = values
            at = pl.ds(l * rc, rc)
            r = lax.dot_general(
                jnp.concatenate([vh, vl], axis=0), dip_hi[at, :], NT, preferred_element_type=f32
            )
            q = lax.dot_general(vh, dip_lo[at, :], NT, preferred_element_type=f32)
            return r[:rows] + r[rows:] + q

        own = split(
            jnp.concatenate([peer_in[par, k, 0:rows, 0:rc] for k in range(sectors)], axis=1)
        )
        ahead = jnp.zeros((rows, rc), f32)
        for l in range(blocks - 1):
            ahead = jnp.where(row_block == l + 1, forward_rows(own, l), ahead)

        @pl.when(has_above)
        def _():
            wait(above_in.at[par, :, pl.ds(0, 2)], sem_z_recv.at[par])

        other = split(jnp.concatenate([above_in[par, k] for k in range(sectors)], axis=1))
        ahead = jnp.where(row_block == 0, forward_rows(other, blocks - 1), ahead)
        ahead = pltpu.roll(ahead, rows - 2, 0)

        def take_e(s, k):
            need, source, out = edge_copy(s)

            @pl.when(need)
            def _():
                wait(edge_in.at[par, source], sem_e_recv.at[par, source])
                out.wait_send()

            return k

        lax.fori_loop(1, sectors, take_e, 0)

        surf = []
        edge = edge_in[par, 0]
        for p in range(2):
            prod = surface_ref[...] * to_col(edge[p : p + 1])
            surf.append(
                [
                    jnp.sum(prod[l * ch : (l + 1) * ch], axis=0, keepdims=True)
                    for l in range(blocks)
                ]
            )
        surf = jnp.concatenate(
            [surf[p][l] for l in range(blocks) for p in range(2)], axis=0
        )

        bound = jnp.zeros((8, width), f32)
        for k in range(sectors):
            bound = bound + edge_in[par, k]
        before = edge_in[par, lax.rem(me + sectors - 1, sectors)]
        after = edge_in[par, lax.rem(me + 1, sectors)]
        lane = lax.broadcasted_iota(jnp.int32, (1, nr), 1)
        for p in (1, 0):
            up, down = channel_copies(par, p)

            @pl.when(has_below)
            def _():
                up.wait_recv()

            @pl.when(has_above)
            def _():
                down.wait_recv()

            gh, gl = split(grid[par, p])
            r = lax.dot_general(mix_split[...], gh, NN, preferred_element_type=f32)
            q = lax.dot_general(mix_split[0:nc, :], gl, NN, preferred_element_type=f32)
            coupled = r[:nc] + r[nc:] + q
            left_row = jnp.where(me == 0, bound[4 + p : 5 + p], before[2 + p : 3 + p])
            right_row = jnp.where(me == sectors - 1, 0.0, after[p : p + 1])
            left_col = to_col(left_row)
            right_col = to_col(right_row)
            x = grid[par, p, ch : ch + nc, :]
            left = jnp.where(lane == 0, left_col, pltpu.roll(x, 1, 1))
            right = jnp.where(lane == nr - 1, right_col, pltpu.roll(x, nr - 1, 1))
            image = diag_ref[...] * x - kinetic_scale * (left + right) + strength * coupled
            value = (factor if p == 1 else -factor) * image
            acc = outer_out[1 - p] + value
            outer_out[1 - p] = acc
            grid[nxt, 1 - p, ch : ch + nc, :] = jnp.where(last, acc, value)
            new_up, new_down = channel_copies(nxt, 1 - p)
            up_old, down_old = channel_copies(par, 1 - p)

            @pl.when(has_above)
            def _():
                up_old.wait_send()

            @pl.when(has_below)
            def _():
                down_old.wait_send()

            @pl.when(jnp.logical_and(has_above, t < STEPS * ORDER - 1))
            def _():
                new_up.start()

            @pl.when(jnp.logical_and(has_below, t < STEPS * ORDER - 1))
            def _():
                new_down.start()


        wait(part_in.at[par, pl.ds(0, sectors - 1)], sem_b_recv.at[par])

        @pl.when(has_below)
        def _():
            wait(below_in.at[par, :, pl.ds(0, 2)], sem_y_recv.at[par])

        near = part_in[par, 0]
        far = below_in[par, 0]
        for k in range(1, sectors):
            near = near + part_in[par, k]
            far = far + below_in[par, k]
        behind = jnp.where(row_block == 0, far, near)
        image = live_ref[...] * (
            energy_rows[...] * c + strength * (ahead + behind) - kinetic_scale * surf
        )
        even = lax.rem(lax.broadcasted_iota(jnp.int32, (rows, 1), 0), 2) == 0
        value = factor * jnp.where(
            even, pltpu.roll(image, rows - 1, 0), -pltpu.roll(image, 1, 0)
        )
        acc = total_inner[...] + value
        total_inner[...] = acc
        term[...] = jnp.where(last, acc, value)

        wait(peer_in.at[par, pl.ds(0, sectors - 1)], sem_a_send)
        wait(part_in.at[par, pl.ds(0, sectors - 1)], sem_b_send)

        @pl.when(has_below)
        def _():
            wait(above_in.at[par, :, pl.ds(0, 2)], sem_z_send)

        @pl.when(has_above)
        def _():
            wait(below_in.at[par, :, pl.ds(0, 2)], sem_y_send)

        return carry

    lax.fori_loop(0, STEPS * ORDER, apply, 0)
    final = total_inner[...]
    for p in range(2):
        inner_out[p] = jnp.concatenate(
            [final[2 * l + p : 2 * l + p + 1] for l in range(blocks)], axis=0
        )


def local(
    planes,
    sectors,
    inner_state,
    outer_state,
    energies,
    dipole,
    surface,
    thresholds,
    coupling_coef,
    coupling_pattern,
    block_sizes,
    field_strength,
):
    blocks, rc, total = dipole.shape
    ch = coupling_coef.shape[1]
    nc, nr = outer_state.shape[1:]
    rows = 2 * blocks
    width = max(rc, -(-nc // 128) * 128)
    vmem = pl.BlockSpec(memory_space=pltpu.VMEM)
    dma = pltpu.SemaphoreType.DMA
    smem = pl.BlockSpec(memory_space=pltpu.SMEM)
    side = -(-ch // 128) * 128
    return pl.pallas_call(
        functools.partial(kernel, planes, sectors, ch),
        out_shape=(
            jax.ShapeDtypeStruct((2, blocks, rc), f32),
            jax.ShapeDtypeStruct((2, nc, nr), f32),
        ),
        in_specs=[vmem] * 3
        + [pl.BlockSpec(memory_space=pltpu.HBM)]
        + [vmem] * 4
        + [smem] * 2,
        out_specs=(vmem, vmem),
        scratch_shapes=[
            pltpu.VMEM((blocks * rc, total), bf16),
            pltpu.VMEM((blocks * rc, total), bf16),
            pltpu.VMEM((2 * nc, nc + 2 * ch), bf16),
            pltpu.VMEM((2, 2, nc + 2 * ch, nr), f32),
            pltpu.VMEM((rows, rc), f32),
            pltpu.VMEM((2, sectors, rows, rc), f32),
            pltpu.VMEM((2, sectors, rows, rc), f32),
            pltpu.VMEM((sectors, rows, rc), f32),
            pltpu.VMEM((2, sectors, rows, rc), f32),
            pltpu.VMEM((2, sectors, rows, rc), f32),
            pltpu.VMEM((blocks + 1, side, side), f32),
            pltpu.VMEM((blocks * rc, total), f32),
            pltpu.VMEM((rows, rc), f32),
            pltpu.VMEM((rows, rc), f32),
            pltpu.VMEM((rows, rc), f32),
            pltpu.VMEM((nc, 1), f32),
            pltpu.VMEM((2, sectors, 8, width), f32),
            dma((sectors,)), dma((2, sectors)),
            dma((blocks,)), dma(()), dma(()),
            dma(()), dma((2,)), dma(()), dma((2,)),
            dma(()), dma((2,)), dma(()), dma((2,)),
            dma((2,)), dma((2, 2)), dma((2,)), dma((2, 2)),
        ],
        compiler_params=pltpu.CompilerParams(
            has_side_effects=True, vmem_limit_bytes=56 * 1024 * 1024
        ),
    )(
        inner_state,
        outer_state,
        energies,
        dipole.reshape(blocks * rc, total),
        surface.reshape(nc, rc),
        thresholds.reshape(1, nc),
        coupling_coef,
        coupling_pattern,
        block_sizes,
        field_strength,
    )


def solution(mesh):
    placed = (
        P(None, "inner", "outer"),
        P(None, "inner", "outer"),
        P("inner", "outer"),
        P("inner", "outer", None),
        P("inner", None, "outer"),
        P("inner"),
        P("inner", None, None),
        P("inner", None, None),
        P("inner"),
        P(),
    )
    return jax.shard_map(
        functools.partial(local, mesh.shape["inner"], mesh.shape["outer"]),
        mesh=mesh,
        in_specs=placed,
        out_specs=(P(None, "inner", "outer"), P(None, "inner", "outer")),
        check_vma=False,
    )
```
